32 devices in a mesh: row: 8 (over y, x, core), col: 4 (over z).
Axes of the slice: x: 2, y: 2, z: 4, core: 2. Of those that a mesh axis runs over, the one named last changes fastest.
Arguments:
- tokens: bfloat16 [256, 8192], P('row', 'col'), may hold values from -6 to 6
- gate_codes: int32 [1024, 28672], P('col', 'row'), may hold values from -2147483648 to 2147483646
- up_codes: int32 [1024, 28672], P('col', 'row'), may hold values from -2147483648 to 2147483646
- down_codes: int32 [3584, 8192], P('row', 'col'), may hold values from -2147483648 to 2147483646
- gate_scales: bfloat16 [64, 28672], P('row'), may hold values from 0.0009994507 to 0.0049743652
- up_scales: bfloat16 [64, 28672], P('row'), may hold values from 0.0009994507 to 0.0049743652
- down_scales: bfloat16 [8192, 224], P('row'), may hold values from 0.00059890747 to 0.0029907227
Outputs:
- mixed: bfloat16 [256, 8192], P('row', 'col')
The draws below stay inside these ranges and needn't reach their ends.
Inputs may be any that keep to these rules, and one draw needn't show every extreme that they name: Every word of gate_codes, up_codes and down_codes is an arbitrary 32-bit pattern: all sixteen codes occur in every nibble position.
All inputs are finite; a program needn't handle non-finite values.
Results may differ from the reference program's by a relative error of at most 0.025.
Values may be sent and summed in bfloat16 or wider, within the bound.
No kernel may reach another device: no remote copies, remote signals or barrier semaphores. Data moves between devices by JAX's collectives and lax.ppermute only.
A program may use at most 192 MiB of HBM per device.

```python
import math
import jax
import jax.numpy as jnp
from jax import lax

D = 8192
FF = 28672
GROUP = 128
TOKENS = 256
N_ROW = 8


def plant(drawn, rng, smallest, high):
    index_at = [jax.random.randint(jax.random.fold_in(rng, axis), (), 0, length) for axis, length in enumerate(drawn.shape)]
    main_axis = drawn.shape.index(max(drawn.shape))
    neighbour = index_at[:main_axis] + [(index_at[main_axis] + 1) % drawn.shape[main_axis]] + index_at[main_axis + 1:]
    return drawn.at[tuple(index_at)].set(smallest).at[tuple(neighbour)].set(high)


def level_of(rng, dims, pieces, least, high):
    def one(dim, blocks):
        draws = jax.random.uniform(jax.random.fold_in(jax.random.fold_in(rng, 6), dim), (blocks,), jnp.float32, least / len(pieces), high / len(pieces))
        return jnp.repeat(jnp.exp(draws), dims[dim] // blocks).reshape((-1,) + (1,) * (len(dims) - dim - 1))

    gain = one(*pieces[0])
    for cut in pieces[1:]:
        gain = gain * one(*cut)
    return gain


def gaussian(rng, extent, deviation, bound, shards=(), held_as=jnp.bfloat16):
    result = jax.random.normal(rng, extent, jnp.float32) * deviation
    if len(shards) > 0:
        result = level_of(rng, extent, shards, -0.22, 0.18) * result
    return jnp.clip(result, min=-bound, max=bound).astype(held_as)


def setup_inputs(seed: int = 0) -> dict:
    streams_of = jax.random.split(jax.random.key(seed), 8)
    return {
        "tokens": gaussian(streams_of[0], (TOKENS, D), 1.0, 6.0, ((0, 8), (1, 4))),
        "gate_codes": plant(jax.random.randint(streams_of[1], (D // 8, FF), -2147483648, 2147483647), jax.random.fold_in(streams_of[1], 1), -2147483648, 2147483646).astype(jnp.int32),
        "up_codes": plant(jax.random.randint(streams_of[2], (D // 8, FF), -2147483648, 2147483647), jax.random.fold_in(streams_of[2], 1), -2147483648, 2147483646).astype(jnp.int32),
        "down_codes": plant(jax.random.randint(streams_of[3], (FF // 8, D), -2147483648, 2147483647), jax.random.fold_in(streams_of[3], 1), -2147483648, 2147483646).astype(jnp.int32),
        "gate_scales": jnp.clip(jnp.exp(math.log(0.0049743652) - 1.6048472 * jax.random.uniform(streams_of[4], (D // GROUP, FF), jnp.float32) ** level_of(streams_of[4], (D // GROUP, FF), ((0, 8),), -0.2, 0.2)), 0.0009994507, 0.0049743652).astype(jnp.bfloat16),
        "up_scales": jnp.clip(jnp.exp(math.log(0.0049743652) - 1.6048472 * jax.random.uniform(streams_of[5], (D // GROUP, FF), jnp.float32) ** level_of(streams_of[5], (D // GROUP, FF), ((0, 8),), -0.2, 0.2)), 0.0009994507, 0.0049743652).astype(jnp.bfloat16),
        "down_scales": jnp.clip(jnp.exp(math.log(0.0029907227) - 1.6081632 * jax.random.uniform(streams_of[6], (D, FF // GROUP), jnp.float32) ** level_of(streams_of[6], (D, FF // GROUP), ((0, 8),), -0.2, 0.2)), 0.00059890747, 0.0029907227).astype(jnp.bfloat16),
    }


def unpack_codes(packed):
    nibbles = [jnp.bitwise_and(jnp.right_shift(packed, 4 * offset), 15) for offset in range(8)]
    stacked = jnp.stack(nibbles, axis=1)
    return stacked.reshape(packed.shape[0] * 8, packed.shape[1]) - 8


def dequantize_rows(packed, scale_rows, group_size):
    values = unpack_codes(packed).astype(jnp.float32)
    columns = values.shape[1]
    shaped = values.reshape(scale_rows.shape[0], group_size, columns) * scale_rows.astype(jnp.float32)[:, None, :]
    return shaped.reshape(values.shape[0], columns).astype(jnp.bfloat16)


def split_cols(array):
    return array.reshape(array.shape[0], N_ROW, array.shape[1] // N_ROW).transpose(1, 0, 2)


def reference(tokens, gate_codes, up_codes, down_codes, gate_scales, up_scales, down_scales):
    down_blocks = down_codes.reshape(N_ROW, down_codes.shape[0] // N_ROW, D)

    def one_block(running, inputs):
        gate_packed, up_packed, gate_scale, up_scale, down_packed, down_scale = inputs
        gate_sum = jnp.dot(tokens, dequantize_rows(gate_packed, gate_scale, GROUP), preferred_element_type=jnp.float32)
        up_sum = jnp.dot(tokens, dequantize_rows(up_packed, up_scale, GROUP), preferred_element_type=jnp.float32)
        hidden = (jax.nn.silu(gate_sum) * up_sum).astype(jnp.bfloat16)
        partial_value = jnp.dot(hidden, dequantize_rows(down_packed, down_scale.T, GROUP), preferred_element_type=jnp.float32).astype(jnp.bfloat16)
        return running + partial_value.astype(jnp.float32), None

    start_sum = jnp.zeros((tokens.shape[0], D), jnp.float32)
    running, unused = lax.scan(one_block, start_sum, (split_cols(gate_codes), split_cols(up_codes), split_cols(gate_scales), split_cols(up_scales), down_blocks, split_cols(down_scales)))
    return running.astype(jnp.bfloat16)
```

```python
import functools

import jax
import jax.numpy as jnp
from jax import lax
from jax.experimental import pallas as pl
from jax.experimental.pallas import tpu as pltpu
from jax.sharding import PartitionSpec as P

GROUP = 128
CODES = 8
WORDS = GROUP // CODES


def tile_of(length, most):
    tile = 128
    for width in range(128, most + 1, 128):
        if length % width == 0:
            tile = width
    return tile


def group_order():
    source = lax.broadcasted_iota(jnp.int32, (GROUP, GROUP), 0)
    target = lax.broadcasted_iota(jnp.int32, (GROUP, GROUP), 1)
    wanted = (target & (WORDS - 1)) * CODES + target // WORDS
    return jnp.where(source == wanted, 1.0, 0.0).astype(jnp.bfloat16)


def unpack_into(codes_ref, scale_ref, dense_ref):
    groups = codes_ref.shape[0] // WORDS
    for g in range(groups):
        words = codes_ref[g * WORDS : (g + 1) * WORDS, :]
        scale = scale_ref[g : g + 1, :]
        flipped = words ^ jnp.int32(-2004318072)
        for k in range(CODES):
            value = flipped if k == CODES - 1 else lax.shift_left(flipped, jnp.int32(28 - 4 * k))
            value = lax.shift_right_arithmetic(value, jnp.int32(28))
            rows = value.astype(jnp.float32).astype(jnp.bfloat16) * scale
            dense_ref[g * GROUP + k * WORDS : g * GROUP + (k + 1) * WORDS, :] = rows


def project_kernel(mine, other, gate_codes, up_codes, gate_scale, up_scale, out, x, gate_dense, up_dense):
    half = mine.shape[0]
    width = gate_codes.shape[1]

    @pl.when(pl.program_id(0) == 0)
    def _():
        order = group_order()
        for g in range(mine.shape[1] // GROUP):
            cols = slice(g * GROUP, (g + 1) * GROUP)
            x[:half, cols] = jnp.dot(mine[:, cols], order, preferred_element_type=jnp.float32).astype(jnp.bfloat16)
            x[half:, cols] = jnp.dot(other[:, cols], order, preferred_element_type=jnp.float32).astype(jnp.bfloat16)

    unpack_into(gate_codes, gate_scale, gate_dense)
    out[:, :width] = jnp.dot(x[...], gate_dense[...], preferred_element_type=jnp.float32).astype(jnp.bfloat16)
    unpack_into(up_codes, up_scale, up_dense)
    out[:, width:] = jnp.dot(x[...], up_dense[...], preferred_element_type=jnp.float32).astype(jnp.bfloat16)


def project(mine, other, gate_codes, up_codes, gate_scale, up_scale):
    words, hidden = gate_codes.shape
    depth = mine.shape[1]
    tokens = 2 * mine.shape[0]
    groups = gate_scale.shape[0]
    width = tile_of(hidden, 512)
    whole = lambda j: (0, 0)
    tile = lambda j: (0, j)
    return pl.pallas_call(
        project_kernel,
        grid=(hidden // width,),
        in_specs=[
            pl.BlockSpec(mine.shape, whole),
            pl.BlockSpec(other.shape, whole),
            pl.BlockSpec((words, width), tile),
            pl.BlockSpec((words, width), tile),
            pl.BlockSpec((groups, width), tile),
            pl.BlockSpec((groups, width), tile),
        ],
        out_specs=pl.BlockSpec((tokens, 2 * width), tile),
        out_shape=jax.ShapeDtypeStruct((tokens, 2 * hidden), jnp.bfloat16),
        scratch_shapes=[
            pltpu.VMEM((tokens, depth), jnp.bfloat16),
            pltpu.VMEM((depth, width), jnp.bfloat16),
            pltpu.VMEM((depth, width), jnp.bfloat16),
        ],
        cost_estimate=pl.CostEstimate(
            flops=4 * tokens * depth * hidden, bytes_accessed=8 * words * hidden, transcendentals=0
        ),
    )(mine, other, gate_codes, up_codes, gate_scale, up_scale)


def hidden_kernel(sums, out):
    width = out.shape[1]
    gate = sums[:, :width].astype(jnp.float32)
    up = sums[:, width:].astype(jnp.float32)
    value = (gate / (1.0 + jnp.exp(-gate)) * up).astype(jnp.bfloat16)
    order = group_order()
    for g in range(width // GROUP):
        cols = slice(g * GROUP, (g + 1) * GROUP)
        out[:, cols] = jnp.dot(value[:, cols], order, preferred_element_type=jnp.float32).astype(jnp.bfloat16)


def activate(sums):
    tokens, columns = sums.shape
    hidden = columns // 2
    width = tile_of(hidden, 512)
    return pl.pallas_call(
        hidden_kernel,
        grid=(hidden // width,),
        in_specs=[pl.BlockSpec((tokens, 2 * width), lambda j: (0, j))],
        out_specs=pl.BlockSpec((tokens, width), lambda j: (0, j)),
        out_shape=jax.ShapeDtypeStruct((tokens, hidden), jnp.bfloat16),
        cost_estimate=pl.CostEstimate(
            flops=2 * tokens * hidden * GROUP, bytes_accessed=6 * tokens * hidden, transcendentals=tokens * hidden
        ),
    )(sums)


def unpack_kernel(codes, scale, out):
    unpack_into(codes, scale, out)


def unpack_down(codes, scale):
    words, columns = codes.shape
    width = tile_of(columns, 256)
    tile = lambda j: (0, j)
    return pl.pallas_call(
        unpack_kernel,
        grid=(columns // width,),
        in_specs=[pl.BlockSpec((words, width), tile), pl.BlockSpec((scale.shape[0], width), tile)],
        out_specs=pl.BlockSpec((words * CODES, width), tile),
        out_shape=jax.ShapeDtypeStruct((words * CODES, columns), jnp.bfloat16),
        cost_estimate=pl.CostEstimate(
            flops=8 * words * CODES * columns, bytes_accessed=20 * words * columns, transcendentals=0
        ),
    )(codes, scale)


def down_kernel(hidden, dense, out):
    out[...] = jnp.dot(hidden[...], dense[...], preferred_element_type=jnp.float32).astype(jnp.bfloat16)


def down(hidden, dense):
    tokens, depth = hidden.shape
    columns = dense.shape[1]
    width = tile_of(columns, 512)
    return pl.pallas_call(
        down_kernel,
        grid=(columns // width,),
        in_specs=[pl.BlockSpec(hidden.shape, lambda j: (0, 0)), pl.BlockSpec((depth, width), lambda j: (0, j))],
        out_specs=pl.BlockSpec((tokens, width), lambda j: (0, j)),
        out_shape=jax.ShapeDtypeStruct((tokens, columns), jnp.bfloat16),
        cost_estimate=pl.CostEstimate(
            flops=2 * tokens * depth * columns, bytes_accessed=2 * depth * columns, transcendentals=0
        ),
    )(hidden, dense)


def swap(value, axis, distance):
    count = lax.axis_size(axis)
    return lax.ppermute(value, axis, [(i, i ^ distance) for i in range(count)])


def input_scales(scales, hidden):
    rows, cols, col = lax.axis_size("row"), lax.axis_size("col"), lax.axis_index("col")
    part = hidden // cols
    sent = jnp.stack(
        [
            jnp.stack([lax.dynamic_slice_in_dim(s, r * hidden + col * part, part, 1) for s in scales])
            for r in range(rows)
        ]
    )
    got = lax.all_to_all(sent, "row", split_axis=0, concat_axis=0, tiled=True)
    own = got.shape[2]
    got = got.reshape(cols, rows // cols, len(scales), own, part)
    got = lax.all_to_all(got, "col", split_axis=0, concat_axis=0, tiled=True)
    got = got.transpose(2, 1, 3, 0, 4).reshape(len(scales), rows // cols * own, hidden)
    return [got[i] for i in range(len(scales))]


def output_scales(scales, model_cols):
    rows, cols, col = lax.axis_size("row"), lax.axis_size("col"), lax.axis_index("col")
    features, groups = scales.shape
    part = features // cols
    mine = lax.dynamic_slice_in_dim(scales, col * part, part, 0).T
    got = lax.all_to_all(
        mine.reshape(rows, groups // rows, part), "row", split_axis=0, concat_axis=0, tiled=True
    )
    got = got.reshape(cols, rows // cols, groups // rows, part)
    got = lax.all_to_all(got, "col", split_axis=0, concat_axis=0, tiled=True)
    return got.transpose(2, 1, 0, 3).reshape(groups // rows, model_cols)


def per_device(tokens, gate_codes, up_codes, down_codes, gate_scales, up_scales, down_scales):
    rows = lax.axis_size("row")
    count = tokens.shape[0]
    mine = jnp.concatenate([tokens] + [swap(tokens, "row", d) for d in range(2, rows, 2)], axis=0)
    other = swap(mine, "row", 1)
    gate_scale, up_scale = input_scales((gate_scales, up_scales), gate_codes.shape[1])
    down_scale = output_scales(down_scales, down_codes.shape[1])
    partial = project(mine, other, gate_codes, up_codes, gate_scale, up_scale)
    down_dense = unpack_down(down_codes, down_scale)
    summed = lax.psum_scatter(partial, "col", scatter_dimension=0, tiled=True)
    hidden = lax.all_gather(activate(summed), "col", axis=0, tiled=True)
    result = down(hidden, down_dense)
    half = result.shape[0] // 2
    received = swap(result[half:], "row", 1)
    pair = (result[:half].astype(jnp.float32) + received.astype(jnp.float32)).astype(jnp.bfloat16)
    pieces = [pair[:count]] + [
        swap(pair[b * count : (b + 1) * count], "row", 2 * b) for b in range(1, rows // 2)
    ]
    total = pieces[0].astype(jnp.float32)
    for piece in pieces[1:]:
        total = total + piece.astype(jnp.float32)
    return total.astype(jnp.bfloat16)


def solution(mesh):
    placed = (
        P("row", "col"),
        P("col", "row"),
        P("col", "row"),
        P("row", "col"),
        P("row", None),
        P("row", None),
        P("row", None),
    )
    return jax.shard_map(
        per_device, mesh=mesh, in_specs=placed, out_specs=P("row", "col"), check_vma=False
    )
```

```python
import functools

import jax
import jax.numpy as jnp
from jax import lax
from jax.experimental import pallas as pl
from jax.experimental.pallas import tpu as pltpu
from jax.sharding import PartitionSpec as P

GROUP = 128
CODES = 8
WORDS = GROUP // CODES


def tile_of(length, most):
    tile = 128
    for width in range(128, most + 1, 128):
        if length % width == 0:
            tile = width
    return tile


def group_order():
    source = lax.broadcasted_iota(jnp.int32, (GROUP, GROUP), 0)
    target = lax.broadcasted_iota(jnp.int32, (GROUP, GROUP), 1)
    wanted = (target & (WORDS - 1)) * CODES + target // WORDS
    return jnp.where(source == wanted, 1.0, 0.0).astype(jnp.bfloat16)


def unpack_into(codes_ref, scale_ref, dense_ref):
    groups = codes_ref.shape[0] // WORDS
    for g in range(groups):
        words = codes_ref[g * WORDS : (g + 1) * WORDS, :]
        scale = scale_ref[g : g + 1, :]
        flipped = words ^ jnp.int32(-2004318072)
        for k in range(CODES):
            value = flipped if k == CODES - 1 else lax.shift_left(flipped, jnp.int32(28 - 4 * k))
            value = lax.shift_right_arithmetic(value, jnp.int32(28))
            rows = value.astype(jnp.float32).astype(jnp.bfloat16) * scale
            dense_ref[g * GROUP + k * WORDS : g * GROUP + (k + 1) * WORDS, :] = rows


def project_kernel(mine, other, gate_codes, up_codes, gate_scale, up_scale, out, x, gate_dense, up_dense):
    half = mine.shape[0]
    width = gate_codes.shape[1]

    @pl.when(pl.program_id(0) == 0)
    def _():
        order = group_order()
        for g in range(mine.shape[1] // GROUP):
            cols = slice(g * GROUP, (g + 1) * GROUP)
            x[:half, cols] = jnp.dot(mine[:, cols], order, preferred_element_type=jnp.float32).astype(jnp.bfloat16)
            x[half:, cols] = jnp.dot(other[:, cols], order, preferred_element_type=jnp.float32).astype(jnp.bfloat16)

    unpack_into(gate_codes, gate_scale, gate_dense)
    out[:, :width] = jnp.dot(x[...], gate_dense[...], preferred_element_type=jnp.float32).astype(jnp.bfloat16)
    unpack_into(up_codes, up_scale, up_dense)
    out[:, width:] = jnp.dot(x[...], up_dense[...], preferred_element_type=jnp.float32).astype(jnp.bfloat16)


def project(mine, other, gate_codes, up_codes, gate_scale, up_scale):
    words, hidden = gate_codes.shape
    depth = mine.shape[1]
    tokens = 2 * mine.shape[0]
    groups = gate_scale.shape[0]
    width = tile_of(hidden, 512)
    whole = lambda j: (0, 0)
    tile = lambda j: (0, j)
    return pl.pallas_call(
        project_kernel,
        grid=(hidden // width,),
        in_specs=[
            pl.BlockSpec(mine.shape, whole),
            pl.BlockSpec(other.shape, whole),
            pl.BlockSpec((words, width), tile),
            pl.BlockSpec((words, width), tile),
            pl.BlockSpec((groups, width), tile),
            pl.BlockSpec((groups, width), tile),
        ],
        out_specs=pl.BlockSpec((tokens, 2 * width), tile),
        out_shape=jax.ShapeDtypeStruct((tokens, 2 * hidden), jnp.bfloat16),
        scratch_shapes=[
            pltpu.VMEM((tokens, depth), jnp.bfloat16),
            pltpu.VMEM((depth, width), jnp.bfloat16),
            pltpu.VMEM((depth, width), jnp.bfloat16),
        ],
        cost_estimate=pl.CostEstimate(
            flops=4 * tokens * depth * hidden, bytes_accessed=8 * words * hidden, transcendentals=0
        ),
    )(mine, other, gate_codes, up_codes, gate_scale, up_scale)


def hidden_kernel(sums, out):
    width = out.shape[1]
    gate = sums[:, :width].astype(jnp.float32)
    up = sums[:, width:].astype(jnp.float32)
    value = (gate / (1.0 + jnp.exp(-gate)) * up).astype(jnp.bfloat16)
    order = group_order()
    for g in range(width // GROUP):
        cols = slice(g * GROUP, (g + 1) * GROUP)
        out[:, cols] = jnp.dot(value[:, cols], order, preferred_element_type=jnp.float32).astype(jnp.bfloat16)


def activate(sums):
    tokens, columns = sums.shape
    hidden = columns // 2
    width = tile_of(hidden, 512)
    return pl.pallas_call(
        hidden_kernel,
        grid=(hidden // width,),
        in_specs=[pl.BlockSpec((tokens, 2 * width), lambda j: (0, j))],
        out_specs=pl.BlockSpec((tokens, width), lambda j: (0, j)),
        out_shape=jax.ShapeDtypeStruct((tokens, hidden), jnp.bfloat16),
        cost_estimate=pl.CostEstimate(
            flops=2 * tokens * hidden * GROUP, bytes_accessed=6 * tokens * hidden, transcendentals=tokens * hidden
        ),
    )(sums)


def unpack_kernel(codes, scale, out):
    unpack_into(codes, scale, out)


def unpack_down(codes, scale):
    words, columns = codes.shape
    width = tile_of(columns, 256)
    tile = lambda j: (0, j)
    return pl.pallas_call(
        unpack_kernel,
        grid=(columns // width,),
        in_specs=[pl.BlockSpec((words, width), tile), pl.BlockSpec((scale.shape[0], width), tile)],
        out_specs=pl.BlockSpec((words * CODES, width), tile),
        out_shape=jax.ShapeDtypeStruct((words * CODES, columns), jnp.bfloat16),
        cost_estimate=pl.CostEstimate(
            flops=8 * words * CODES * columns, bytes_accessed=20 * words * columns, transcendentals=0
        ),
    )(codes, scale)


def down_kernel(hidden, dense, out):
    out[...] = jnp.dot(hidden[...], dense[...], preferred_element_type=jnp.float32).astype(jnp.bfloat16)


def down(hidden, dense):
    tokens, depth = hidden.shape
    columns = dense.shape[1]
    width = tile_of(columns, 512)
    return pl.pallas_call(
        down_kernel,
        grid=(columns // width,),
        in_specs=[pl.BlockSpec(hidden.shape, lambda j: (0, 0)), pl.BlockSpec((depth, width), lambda j: (0, j))],
        out_specs=pl.BlockSpec((tokens, width), lambda j: (0, j)),
        out_shape=jax.ShapeDtypeStruct((tokens, columns), jnp.bfloat16),
        cost_estimate=pl.CostEstimate(
            flops=2 * tokens * depth * columns, bytes_accessed=2 * depth * columns, transcendentals=0
        ),
    )(hidden, dense)


def swap(value, axis, distance):
    count = lax.axis_size(axis)
    return lax.ppermute(value, axis, [(i, i ^ distance) for i in range(count)])


def input_scales(scales, hidden):
    rows, cols, col = lax.axis_size("row"), lax.axis_size("col"), lax.axis_index("col")
    part = hidden // cols
    sent = jnp.stack(
        [
            jnp.stack([lax.dynamic_slice_in_dim(s, r * hidden + col * part, part, 1) for s in scales])
            for r in range(rows)
        ]
    )
    got = lax.all_to_all(sent, "row", split_axis=0, concat_axis=0, tiled=True)
    own = got.shape[2]
    got = got.reshape(cols, rows // cols, len(scales), own, part)
    got = lax.all_to_all(got, "col", split_axis=0, concat_axis=0, tiled=True)
    got = got.transpose(2, 1, 3, 0, 4).reshape(len(scales), rows // cols * own, hidden)
    return [got[i] for i in range(len(scales))]


def output_scales(scales, model_cols):
    rows, cols, col = lax.axis_size("row"), lax.axis_size("col"), lax.axis_index("col")
    features, groups = scales.shape
    part = features // cols
    mine = lax.dynamic_slice_in_dim(scales, col * part, part, 0).T
    got = lax.all_to_all(
        mine.reshape(rows, groups // rows, part), "row", split_axis=0, concat_axis=0, tiled=True
    )
    got = got.reshape(cols, rows // cols, groups // rows, part)
    got = lax.all_to_all(got, "col", split_axis=0, concat_axis=0, tiled=True)
    return got.transpose(2, 1, 0, 3).reshape(groups // rows, model_cols)


VMEM = pl.BlockSpec(memory_space=pltpu.VMEM)
SMEM = pl.BlockSpec(memory_space=pltpu.SMEM)


def local(kernel, shapes, *args, scalars=0, scratch=(), flops=0, limit=16):
    several = isinstance(shapes, list)
    return pl.pallas_call(
        kernel,
        in_specs=[SMEM] * scalars + [VMEM] * (len(args) - scalars),
        out_specs=[VMEM] * len(shapes) if several else VMEM,
        out_shape=shapes,
        scratch_shapes=list(scratch),
        compiler_params=pltpu.CompilerParams(vmem_limit_bytes=limit << 20),
        cost_estimate=pl.CostEstimate(flops=flops, bytes_accessed=0, transcendentals=0),
    )(*args)


def bf16(*shape):
    return jax.ShapeDtypeStruct(shape, jnp.bfloat16)


def slot_orders(col):
    table = jnp.array([[3, 2, 1, 0], [3, 2, 0, 1], [0, 1, 3, 2], [0, 1, 2, 3]], jnp.int32)
    return lax.dynamic_slice_in_dim(table, col, 1, 0)[0]


def inward(value):
    return lax.ppermute(value, "col", [(0, 1), (3, 2)])


def across(value):
    return lax.ppermute(value, "col", [(1, 2), (2, 1)])


def outward(value):
    return lax.ppermute(value, "col", [(2, 3), (1, 0)])


def lanes_at(start, size):
    return pl.ds(pl.multiple_of(start, 128), size)


def dot(a, b):
    return jnp.dot(a, b, preferred_element_type=jnp.float32)


CHIP, CORE, COL, ORDER = 0, 1, 2, 3


def first_kernel(at, tokens, gate, up, *outs, part):
    count, own = tokens.shape[0], gate.shape[0]
    order = group_order()
    for g in range(tokens.shape[1] // GROUP):
        lanes = slice(g * GROUP, (g + 1) * GROUP)
        value = dot(tokens[:, lanes], order).astype(jnp.bfloat16)
        for out in outs:
            out[:count, lanes] = value
    for j, out in enumerate(outs):
        for core in range(2):
            start = (((at[CHIP] ^ j) * 2 + core) * 4 + at[ORDER]) * part
            out[count : count + own, core * part : (core + 1) * part] = gate[:, lanes_at(start, part)]
            out[count + own :, core * part : (core + 1) * part] = up[:, lanes_at(start, part)]


def second_kernel(at, gate, up, down_t, *outs, part):
    own = gate.shape[0]
    groups, width = down_t.shape[1:]
    for j, out in enumerate(outs):
        for core in range(2):
            for slot in range(1, 4):
                start = (((at[CHIP] ^ j) * 2 + core) * 4 + at[ORDER + slot]) * part
                lanes = slice(((slot - 1) * 2 + core) * part, ((slot - 1) * 2 + core + 1) * part)
                out[:own, lanes] = gate[:, lanes_at(start, part)]
                out[own:, lanes] = up[:, lanes_at(start, part)]
        for i in range(0, groups, 2 * own):
            count = min(2 * own, groups - i)
            lanes = slice(6 * part + i // (2 * own) * width, 6 * part + (i // (2 * own) + 1) * width)
            out[:count, lanes] = down_t[at[CHIP] ^ j, i : i + count, :]


def gather_kernel(at, mine, other, x, gate, up, *, count, part):
    block = mine.shape[0] // 4
    half = x.shape[0] // 2
    own = gate.shape[1]
    for j in range(4):
        x[j * count : (j + 1) * count, :] = mine[j * block : j * block + count, :]
        x[half + j * count : half + (j + 1) * count, :] = other[j * block : j * block + count, :]
    source = (at[CHIP] ^ at[COL]) * block + count
    rows = pl.ds(pl.multiple_of(source, 16), 2 * own)
    lanes = lanes_at(at[CORE] * part, part)
    for core, ref in ((at[CORE], mine), (1 - at[CORE], other)):
        both = ref[rows, lanes]
        gate[core] = both[:own]
        up[core] = both[own:]


def pick_kernel(at, own, *refs):
    received, out = refs[:-1], refs[-1]
    keep = at[CHIP] == at[COL]

    @pl.when(keep)
    def _():
        out[...] = own[...]

    @pl.when(jnp.logical_not(keep))
    def _():
        total = received[0][...]
        for ref in received[1:]:
            total += ref[...]
        out[...] = total


def spread_kernel(at, mine, other, gate, up, down_scale, *, part):
    own = gate.shape[2]
    groups, features = down_scale.shape
    width = features // 2
    for core, ref in ((at[CORE], mine), (1 - at[CORE], other)):
        for slot in range(3):
            lanes = lanes_at((slot * 2 + at[CORE]) * part, part)
            gate[slot, core] = ref[:own, lanes]
            up[slot, core] = ref[own:, lanes]
        rows = []
        for i in range(0, 2 * groups, 2 * own):
            start = 6 * part + i // (2 * own) * width
            rows.append(ref[: min(2 * own, 2 * groups - i), start : start + width].astype(jnp.float32))
        rows = jnp.concatenate(rows, axis=0)
        value = jnp.where(at[CORE] == 0, rows[:groups], rows[groups:])
        down_scale[:, lanes_at(core * width, width)] = value.astype(jnp.bfloat16)


def unpack_tile(codes, scale, groups, dense):
    for g in range(groups):
        words = codes(g) ^ jnp.int32(-2004318072)
        for k in range(CODES):
            value = words if k == CODES - 1 else lax.shift_left(words, jnp.int32(28 - 4 * k))
            value = lax.shift_right_arithmetic(value, jnp.int32(28))
            rows = slice(g * GROUP + k * WORDS, g * GROUP + (k + 1) * WORDS)
            dense[rows, :] = value.astype(jnp.float32).astype(jnp.bfloat16) * scale(g)


def shard_kernel(at, x, gate_codes, up_codes, gate_scale, up_scale, out, *dense, slot, index):
    part = gate_codes.shape[1] // 4
    own = gate_scale.shape[-2]
    groups = gate_codes.shape[0] // WORDS
    lanes = lanes_at(at[ORDER + slot] * part, part)
    for i, (codes, scale) in enumerate(((gate_codes, gate_scale), (up_codes, up_scale))):
        where = () if index is None else (index,)
        unpack_tile(
            lambda g: codes[g * WORDS : (g + 1) * WORDS, lanes],
            lambda g: scale[where + (g // own, slice(g % own, g % own + 1), slice(None))],
            groups,
            dense[i],
        )
        out[:, i * part : (i + 1) * part] = dot(x[...], dense[i][...]).astype(jnp.bfloat16)


def project_shard(at, slot, x, gate_codes, up_codes, gate_scale, up_scale):
    tokens, depth = x.shape
    part = gate_codes.shape[1] // 4
    index = None if slot == 0 else slot - 1
    return local(
        functools.partial(shard_kernel, slot=slot, index=index),
        bf16(tokens, 2 * part),
        at, x, gate_codes, up_codes, gate_scale, up_scale,
        scalars=1,
        scratch=[pltpu.VMEM((depth, part), jnp.bfloat16)] * 2,
        flops=tokens * depth * part // 4,
        limit=20,
    )


def plus_kernel(a, b, out):
    out[...] = (a[...].astype(jnp.float32) + b[...].astype(jnp.float32)).astype(jnp.bfloat16)


def plus(a, b):
    return local(plus_kernel, bf16(*a.shape), a, b, flops=a.size)


def final_kernel(a, b, c, d, out):
    width = out.shape[1]
    order = group_order()
    for g in range(width // GROUP):
        gate_at = slice(g * GROUP, (g + 1) * GROUP)
        up_at = slice(width + g * GROUP, width + (g + 1) * GROUP)
        gate, up = (
            a[:, at].astype(jnp.float32)
            + b[:, at].astype(jnp.float32)
            + c[:, at].astype(jnp.float32)
            + d[:, at].astype(jnp.float32)
            for at in (gate_at, up_at)
        )
        value = (gate / (1.0 + jnp.exp(-gate)) * up).astype(jnp.bfloat16)
        out[:, gate_at] = dot(value, order).astype(jnp.bfloat16)


def down_kernel_of(slot, parts, begin, last):
    def kernel(at, *refs):
        refs = list(refs)
        hidden, (codes, scale), refs = refs[:parts], refs[parts : parts + 2], refs[parts + 2 :]
        before = None if begin else refs.pop(0)
        dense, outs = refs[-1], refs[:-1]
        value = hidden[0][...]
        for ref in hidden[1:]:
            value = value + ref[...]
        depth = value.shape[1]
        words, groups = depth // CODES, depth // GROUP
        columns = codes.shape[1]
        half = value.shape[0] // 2
        first = at[ORDER + slot]
        for start in range(0, columns, columns // 4):
            lanes = slice(start, start + columns // 4)
            unpack_tile(
                lambda g: codes[pl.ds(pl.multiple_of(first * words + g * WORDS, WORDS), WORDS), lanes],
                lambda g: scale[first, g : g + 1, lanes],
                groups,
                dense.at[:, lanes],
            )
            total = dot(value, dense[:, lanes])
            if before is not None:
                total += before[:, lanes]
            if last:
                outs[0][:, lanes] = total[:half].astype(jnp.bfloat16)
                outs[1][:, lanes] = total[half:].astype(jnp.bfloat16)
            else:
                outs[0][:, lanes] = total

    return kernel


def down_shard(at, slot, hidden, codes, scale, before=None, last=False):
    tokens, depth = hidden[0].shape
    columns = codes.shape[1]
    if last:
        shapes = [bf16(tokens // 2, columns)] * 2
    else:
        shapes = jax.ShapeDtypeStruct((tokens, columns), jnp.float32)
    extra = () if before is None else (before,)
    return local(
        down_kernel_of(slot, len(hidden), before is None, last),
        shapes,
        at, *hidden, codes, scale, *extra,
        scalars=1,
        scratch=[pltpu.VMEM((depth, columns), jnp.bfloat16)],
        flops=tokens * depth * columns // 4,
    )


def pair_kernel(left, right, *outs):
    count = outs[0].shape[0]
    for b, out in enumerate(outs):
        rows = slice(b * count, (b + 1) * count)
        out[...] = (left[rows].astype(jnp.float32) + right[rows].astype(jnp.float32)).astype(jnp.bfloat16)


def total_kernel(*refs):
    total = refs[0][...].astype(jnp.float32)
    for ref in refs[1:-1]:
        total += ref[...].astype(jnp.float32)
    refs[-1][...] = total.astype(jnp.bfloat16)


def line_device(tokens, gate_codes, up_codes, down_codes, gate_scales, up_scales, down_scales):
    rows, cols = lax.axis_size("row"), lax.axis_size("col")
    row, col = lax.axis_index("row"), lax.axis_index("col")
    count, depth = tokens.shape
    own, hidden_units = gate_scales.shape[0], gate_codes.shape[1]
    part = hidden_units // cols
    features = down_codes.shape[1]
    down_groups = down_scales.shape[1] // rows
    at = jnp.concatenate([jnp.stack([row // 2, row % 2, col]).astype(jnp.int32), slot_orders(col)])

    first = local(
        functools.partial(first_kernel, part=part),
        [bf16(count + 2 * own, depth)] * 4,
        at, tokens, gate_scales, up_scales,
        scalars=1,
    )
    mine = jnp.concatenate([first[0]] + [swap(first[j], "row", 2 * j) for j in range(1, 4)], axis=0)
    other = swap(mine, "row", 1)
    scale = bf16(2, own, part)
    x, gate_scale, up_scale = local(
        functools.partial(gather_kernel, count=count, part=part),
        [bf16(rows * count, depth), scale, scale],
        at, mine, other,
        scalars=1,
    )

    down_t = down_scales.T.reshape(rows // 2, 2 * down_groups, down_scales.shape[0])
    pieces = -(-down_groups // own)
    second = local(
        functools.partial(second_kernel, part=part),
        [bf16(2 * own, 6 * part + pieces * down_scales.shape[0])] * 4,
        at, gate_scales, up_scales, down_t,
        scalars=1,
    )
    received = []
    for j in range(1, 4):
        pairs = [(r * cols + r // 2, (r ^ (2 * j)) * cols + r // 2) for r in range(rows)]
        received.append(lax.ppermute(second[j], ("row", "col"), pairs))
    second = local(pick_kernel, bf16(*second[0].shape), at, second[0], *received, scalars=1)
    scale = bf16(3, 2, own, part)
    gate_rest, up_rest, down_scale = local(
        functools.partial(spread_kernel, part=part),
        [scale, scale, bf16(down_groups, features)],
        at, second, swap(second, "row", 1),
        scalars=1,
    )
    down_scale = down_scale.reshape(cols, down_groups // cols, features)

    far = project_shard(at, 0, x, gate_codes, up_codes, gate_scale, up_scale)
    far_in = inward(far)
    inner = project_shard(at, 1, x, gate_codes, up_codes, gate_rest, up_rest)
    inner_in = inward(inner)
    near = project_shard(at, 2, x, gate_codes, up_codes, gate_rest, up_rest)
    near_in = inward(near)
    mine_sum = project_shard(at, 3, x, gate_codes, up_codes, gate_rest, up_rest)
    far_across = across(plus(far, far_in))
    inner_across = across(plus(inner, inner_in))
    far_out = outward(plus(near, far_across))
    hidden = local(
        final_kernel,
        bf16(rows * count, part),
        mine_sum, near_in, inner_across, far_out,
        flops=rows * count * part * GROUP // 4,
    )

    to_inner = inward(hidden)
    between = across(hidden)
    to_outer = outward(hidden)
    second_across = across(to_inner)
    to_outer2 = outward(between)
    to_outer3 = outward(second_across)
    total = down_shard(at, 3, [hidden], down_codes, down_scale)
    total = down_shard(at, 2, [to_inner, to_outer], down_codes, down_scale, total)
    total = down_shard(at, 1, [between, to_outer2], down_codes, down_scale, total)
    left, right = down_shard(at, 0, [second_across, to_outer3], down_codes, down_scale, total, last=True)

    pair = local(pair_kernel, [bf16(count, features)] * 4, left, swap(right, "row", 1))
    return local(
        total_kernel,
        bf16(count, features),
        pair[0], *[swap(pair[b], "row", 2 * b) for b in range(1, 4)],
    )


def per_device(tokens, gate_codes, up_codes, down_codes, gate_scales, up_scales, down_scales):
    rows, cols = lax.axis_size("row"), lax.axis_size("col")
    sizes = (gate_codes.shape[1], down_scales.shape[0])
    fits = 2 * gate_codes.shape[1] <= tokens.shape[1] * cols and tokens.shape[0] % 16 == 0
    if cols == 4 and rows == 2 * cols and fits and all(n % (cols * 128) == 0 for n in sizes):
        return line_device(tokens, gate_codes, up_codes, down_codes, gate_scales, up_scales, down_scales)
    count = tokens.shape[0]
    mine = jnp.concatenate([tokens] + [swap(tokens, "row", d) for d in range(2, rows, 2)], axis=0)
    other = swap(mine, "row", 1)
    gate_scale, up_scale = input_scales((gate_scales, up_scales), gate_codes.shape[1])
    down_scale = output_scales(down_scales, down_codes.shape[1])
    partial = project(mine, other, gate_codes, up_codes, gate_scale, up_scale)
    down_dense = unpack_down(down_codes, down_scale)
    summed = lax.psum_scatter(partial, "col", scatter_dimension=0, tiled=True)
    hidden = lax.all_gather(activate(summed), "col", axis=0, tiled=True)
    result = down(hidden, down_dense)
    half = result.shape[0] // 2
    received = swap(result[half:], "row", 1)
    pair = (result[:half].astype(jnp.float32) + received.astype(jnp.float32)).astype(jnp.bfloat16)
    pieces = [pair[:count]] + [
        swap(pair[b * count : (b + 1) * count], "row", 2 * b) for b in range(1, rows // 2)
    ]
    total = pieces[0].astype(jnp.float32)
    for piece in pieces[1:]:
        total = total + piece.astype(jnp.float32)
    return total.astype(jnp.bfloat16)


def solution(mesh):
    placed = (
        P("row", "col"),
        P("col", "row"),
        P("col", "row"),
        P("row", "col"),
        P("row", None),
        P("row", None),
        P("row", None),
    )
    return jax.shard_map(
        per_device, mesh=mesh, in_specs=placed, out_specs=P("row", "col"), check_vma=False
    )
```

```python
import functools

import jax
import jax.numpy as jnp
from jax import lax
from jax.experimental import pallas as pl
from jax.experimental.pallas import tpu as pltpu
from jax.sharding import PartitionSpec as P


GROUP = 128
CODES = 8
WORDS = GROUP // CODES


def tile_of(length, most):
    tile = 128
    for width in range(128, most + 1, 128):
        if length % width == 0:
            tile = width
    return tile


def group_order():
    source = lax.broadcasted_iota(jnp.int32, (GROUP, GROUP), 0)
    target = lax.broadcasted_iota(jnp.int32, (GROUP, GROUP), 1)
    wanted = (target & (WORDS - 1)) * CODES + target // WORDS
    return jnp.where(source == wanted, 1.0, 0.0).astype(jnp.bfloat16)


def unpack_into(codes_ref, scale_ref, dense_ref):
    groups = codes_ref.shape[0] // WORDS
    for g in range(groups):
        words = codes_ref[g * WORDS : (g + 1) * WORDS, :]
        scale = scale_ref[g : g + 1, :]
        flipped = words ^ jnp.int32(-2004318072)
        for k in range(CODES):
            value = flipped if k == CODES - 1 else lax.shift_left(flipped, jnp.int32(28 - 4 * k))
            value = lax.shift_right_arithmetic(value, jnp.int32(28))
            rows = value.astype(jnp.float32).astype(jnp.bfloat16) * scale
            dense_ref[g * GROUP + k * WORDS : g * GROUP + (k + 1) * WORDS, :] = rows


def project_kernel(mine, other, gate_codes, up_codes, gate_scale, up_scale, out, x, gate_dense, up_dense):
    half = mine.shape[0]
    width = gate_codes.shape[1]

    @pl.when(pl.program_id(0) == 0)
    def _():
        order = group_order()
        for g in range(mine.shape[1] // GROUP):
            cols = slice(g * GROUP, (g + 1) * GROUP)
            x[:half, cols] = jnp.dot(mine[:, cols], order, preferred_element_type=jnp.float32).astype(jnp.bfloat16)
            x[half:, cols] = jnp.dot(other[:, cols], order, preferred_element_type=jnp.float32).astype(jnp.bfloat16)

    unpack_into(gate_codes, gate_scale, gate_dense)
    out[:, :width] = jnp.dot(x[...], gate_dense[...], preferred_element_type=jnp.float32).astype(jnp.bfloat16)
    unpack_into(up_codes, up_scale, up_dense)
    out[:, width:] = jnp.dot(x[...], up_dense[...], preferred_element_type=jnp.float32).astype(jnp.bfloat16)


def project(mine, other, gate_codes, up_codes, gate_scale, up_scale):
    words, hidden = gate_codes.shape
    depth = mine.shape[1]
    tokens = 2 * mine.shape[0]
    groups = gate_scale.shape[0]
    width = tile_of(hidden, 512)
    whole = lambda j: (0, 0)
    tile = lambda j: (0, j)
    return pl.pallas_call(
        project_kernel,
        grid=(hidden // width,),
        in_specs=[
            pl.BlockSpec(mine.shape, whole),
            pl.BlockSpec(other.shape, whole),
            pl.BlockSpec((words, width), tile),
            pl.BlockSpec((words, width), tile),
            pl.BlockSpec((groups, width), tile),
            pl.BlockSpec((groups, width), tile),
        ],
        out_specs=pl.BlockSpec((tokens, 2 * width), tile),
        out_shape=jax.ShapeDtypeStruct((tokens, 2 * hidden), jnp.bfloat16),
        scratch_shapes=[
            pltpu.VMEM((tokens, depth), jnp.bfloat16),
            pltpu.VMEM((depth, width), jnp.bfloat16),
            pltpu.VMEM((depth, width), jnp.bfloat16),
        ],
        cost_estimate=pl.CostEstimate(
            flops=4 * tokens * depth * hidden, bytes_accessed=8 * words * hidden, transcendentals=0
        ),
    )(mine, other, gate_codes, up_codes, gate_scale, up_scale)


def hidden_kernel(sums, out):
    width = out.shape[1]
    gate = sums[:, :width].astype(jnp.float32)
    up = sums[:, width:].astype(jnp.float32)
    value = (gate / (1.0 + jnp.exp(-gate)) * up).astype(jnp.bfloat16)
    order = group_order()
    for g in range(width // GROUP):
        cols = slice(g * GROUP, (g + 1) * GROUP)
        out[:, cols] = jnp.dot(value[:, cols], order, preferred_element_type=jnp.float32).astype(jnp.bfloat16)


def activate(sums):
    tokens, columns = sums.shape
    hidden = columns // 2
    width = tile_of(hidden, 512)
    return pl.pallas_call(
        hidden_kernel,
        grid=(hidden // width,),
        in_specs=[pl.BlockSpec((tokens, 2 * width), lambda j: (0, j))],
        out_specs=pl.BlockSpec((tokens, width), lambda j: (0, j)),
        out_shape=jax.ShapeDtypeStruct((tokens, hidden), jnp.bfloat16),
        cost_estimate=pl.CostEstimate(
            flops=2 * tokens * hidden * GROUP, bytes_accessed=6 * tokens * hidden, transcendentals=tokens * hidden
        ),
    )(sums)


def unpack_kernel(codes, scale, out):
    unpack_into(codes, scale, out)


def unpack_down(codes, scale):
    words, columns = codes.shape
    width = tile_of(columns, 256)
    tile = lambda j: (0, j)
    return pl.pallas_call(
        unpack_kernel,
        grid=(columns // width,),
        in_specs=[pl.BlockSpec((words, width), tile), pl.BlockSpec((scale.shape[0], width), tile)],
        out_specs=pl.BlockSpec((words * CODES, width), tile),
        out_shape=jax.ShapeDtypeStruct((words * CODES, columns), jnp.bfloat16),
        cost_estimate=pl.CostEstimate(
            flops=8 * words * CODES * columns, bytes_accessed=20 * words * columns, transcendentals=0
        ),
    )(codes, scale)


def down_kernel(hidden, dense, out):
    out[...] = jnp.dot(hidden[...], dense[...], preferred_element_type=jnp.float32).astype(jnp.bfloat16)


def down(hidden, dense):
    tokens, depth = hidden.shape
    columns = dense.shape[1]
    width = tile_of(columns, 512)
    return pl.pallas_call(
        down_kernel,
        grid=(columns // width,),
        in_specs=[pl.BlockSpec(hidden.shape, lambda j: (0, 0)), pl.BlockSpec((depth, width), lambda j: (0, j))],
        out_specs=pl.BlockSpec((tokens, width), lambda j: (0, j)),
        out_shape=jax.ShapeDtypeStruct((tokens, columns), jnp.bfloat16),
        cost_estimate=pl.CostEstimate(
            flops=2 * tokens * depth * columns, bytes_accessed=2 * depth * columns, transcendentals=0
        ),
    )(hidden, dense)


def swap(value, axis, distance):
    count = lax.axis_size(axis)
    return lax.ppermute(value, axis, [(i, i ^ distance) for i in range(count)])


def input_scales(scales, hidden):
    rows, cols, col = lax.axis_size("row"), lax.axis_size("col"), lax.axis_index("col")
    part = hidden // cols
    sent = jnp.stack(
        [
            jnp.stack([lax.dynamic_slice_in_dim(s, r * hidden + col * part, part, 1) for s in scales])
            for r in range(rows)
        ]
    )
    got = lax.all_to_all(sent, "row", split_axis=0, concat_axis=0, tiled=True)
    own = got.shape[2]
    got = got.reshape(cols, rows // cols, len(scales), own, part)
    got = lax.all_to_all(got, "col", split_axis=0, concat_axis=0, tiled=True)
    got = got.transpose(2, 1, 3, 0, 4).reshape(len(scales), rows // cols * own, hidden)
    return [got[i] for i in range(len(scales))]


def output_scales(scales, model_cols):
    rows, cols, col = lax.axis_size("row"), lax.axis_size("col"), lax.axis_index("col")
    features, groups = scales.shape
    part = features // cols
    mine = lax.dynamic_slice_in_dim(scales, col * part, part, 0).T
    got = lax.all_to_all(
        mine.reshape(rows, groups // rows, part), "row", split_axis=0, concat_axis=0, tiled=True
    )
    got = got.reshape(cols, rows // cols, groups // rows, part)
    got = lax.all_to_all(got, "col", split_axis=0, concat_axis=0, tiled=True)
    return got.transpose(2, 1, 0, 3).reshape(groups // rows, model_cols)


VMEM = pl.BlockSpec(memory_space=pltpu.VMEM)
SMEM = pl.BlockSpec(memory_space=pltpu.SMEM)
HBM = pl.BlockSpec(memory_space=pltpu.HBM)


def local(kernel, shapes, *args, scalars=0, remote=0, scratch=(), flops=0, limit=16):
    several = isinstance(shapes, list)
    args = list(args)
    for i in range(scalars, scalars + remote):
        args[i] = pltpu.with_memory_space_constraint(args[i], pltpu.HBM)
    return pl.pallas_call(
        kernel,
        in_specs=[SMEM] * scalars + [HBM] * remote + [VMEM] * (len(args) - scalars - remote),
        out_specs=[VMEM] * len(shapes) if several else VMEM,
        out_shape=shapes,
        scratch_shapes=list(scratch),
        compiler_params=pltpu.CompilerParams(vmem_limit_bytes=limit << 20),
        cost_estimate=pl.CostEstimate(flops=flops, bytes_accessed=0, transcendentals=0),
    )(*args)


def bf16(*shape):
    return jax.ShapeDtypeStruct(shape, jnp.bfloat16)


def inward(value):
    return lax.ppermute(value, "col", [(0, 1), (3, 2)])


def across(value):
    return lax.ppermute(value, "col", [(1, 2), (2, 1)])


def outward(value):
    return lax.ppermute(value, "col", [(2, 3), (1, 0)])


def ends(value):
    return lax.ppermute(value, "col", [(0, 3), (3, 0)])


def lanes_at(start, size):
    return pl.ds(pl.multiple_of(start, 128), size)


def dot(a, b):
    return jnp.dot(a, b, preferred_element_type=jnp.float32)


CHIP, CORE, COL = 0, 1, 2

MASKS = (2, 3, 1, 0)


def first_kernel(at, tokens, gate, up, *refs, part):
    outs, (held, arrived, sems) = refs[:4], refs[4:]
    count, own = tokens.shape[0], gate.shape[0]
    fetch = pltpu.make_async_copy(tokens, held, arrived)
    fetch.start()
    copies = []
    for j, out in enumerate(outs):
        for core in range(2):
            start = (((at[CHIP] ^ j) * 2 + core) * 4 + (at[COL] ^ MASKS[0])) * part
            for i, scale in enumerate((gate, up)):
                rows = slice(count + i * own, count + (i + 1) * own)
                copies.append(
                    pltpu.make_async_copy(
                        scale.at[:, lanes_at(start, part)],
                        out.at[rows, core * part : (core + 1) * part],
                        sems.at[len(copies)],
                    )
                )
                copies[-1].start()
    order = group_order()
    fetch.wait()
    for g in range(tokens.shape[1] // GROUP):
        lanes = slice(g * GROUP, (g + 1) * GROUP)
        value = dot(held[:, lanes], order).astype(jnp.bfloat16)
        for out in outs:
            out[:count, lanes] = value
    for copy in copies:
        copy.wait()


def second_kernel(at, gate, up, *refs, part):
    outs, sems = refs[:-1], refs[-1]
    own = gate.shape[0]
    copies = []
    for j, out in enumerate(outs):
        for core in range(2):
            for slot in range(1, 4):
                start = (((at[CHIP] ^ j) * 2 + core) * 4 + (at[COL] ^ MASKS[slot])) * part
                lanes = slice(((slot - 1) * 2 + core) * part, ((slot - 1) * 2 + core + 1) * part)
                for i, scale in enumerate((gate, up)):
                    copies.append(
                        pltpu.make_async_copy(
                            scale.at[:, lanes_at(start, part)],
                            out.at[i * own : (i + 1) * own, lanes],
                            sems.at[len(copies)],
                        )
                    )
                    copies[-1].start()
    for copy in copies:
        copy.wait()


def third_kernel(at, down_t, *outs):
    for j, out in enumerate(outs):
        out[...] = down_t[at[CHIP] ^ j]


def stage_kernel(at, gate, up, *refs):
    outs, sems = refs[:-1], refs[-1]
    part = gate.shape[1] // 4
    copies = []
    for slot, mask in enumerate(MASKS):
        lanes = lanes_at((at[COL] ^ mask) * part, part)
        for i, codes in enumerate((gate, up)):
            index = 2 * slot + i
            copies.append(pltpu.make_async_copy(codes.at[:, lanes], outs[index], sems.at[index]))
            copies[-1].start()
    for copy in copies:
        copy.wait()


def gather_kernel(at, mine, other, x, gate, up, *, count, part):
    block = mine.shape[0] // 4
    half = x.shape[0] // 2
    own = gate.shape[1]
    for j in range(4):
        x[j * count : (j + 1) * count, :] = mine[j * block : j * block + count, :]
        x[half + j * count : half + (j + 1) * count, :] = other[j * block : j * block + count, :]
    source = (at[CHIP] ^ at[COL]) * block + count
    rows = pl.ds(pl.multiple_of(source, 16), 2 * own)
    lanes = lanes_at(at[CORE] * part, part)
    for core, ref in ((at[CORE], mine), (1 - at[CORE], other)):
        both = ref[rows, lanes]
        gate[core] = both[:own]
        up[core] = both[own:]


def pick_kernel(at, own, *refs):
    received, out = refs[:-1], refs[-1]
    keep = at[CHIP] == at[COL]

    @pl.when(keep)
    def _():
        out[...] = own[...]

    @pl.when(jnp.logical_not(keep))
    def _():
        total = received[0][...]
        for ref in received[1:]:
            total += ref[...]
        out[...] = total


def spread_kernel(at, mine, other, gate, up, *, part):
    own = gate.shape[2]
    for core, ref in ((at[CORE], mine), (1 - at[CORE], other)):
        for slot in range(3):
            lanes = lanes_at((slot * 2 + at[CORE]) * part, part)
            gate[slot, core] = ref[:own, lanes]
            up[slot, core] = ref[own:, lanes]


def spread_down_kernel(at, mine, other, out):
    shards, groups, features = out.shape
    width = features // 2
    for core, ref in ((at[CORE], mine), (1 - at[CORE], other)):
        rows = ref[...].astype(jnp.float32)
        value = jnp.where(at[CORE] == 0, rows[: shards * groups], rows[shards * groups :]).astype(jnp.bfloat16)
        for shard in range(shards):
            out[shard, :, lanes_at(core * width, width)] = value[shard * groups : (shard + 1) * groups]


def unpack_tile(codes, scale, groups, dense):
    for g in range(groups):
        words = codes(g) ^ jnp.int32(-2004318072)
        for k in range(CODES):
            value = words if k == CODES - 1 else lax.shift_left(words, jnp.int32(28 - 4 * k))
            value = lax.shift_right_arithmetic(value, jnp.int32(28))
            rows = slice(g * GROUP + k * WORDS, g * GROUP + (k + 1) * WORDS)
            dense[rows, :] = value.astype(jnp.float32).astype(jnp.bfloat16) * scale(g)


def shard_kernel(x, gate_codes, up_codes, gate_scale, up_scale, out, *dense, index):
    part = gate_codes.shape[1]
    own = gate_scale.shape[-2]
    groups = gate_codes.shape[0] // WORDS
    where = () if index is None else (index,)
    for i, (codes, scale) in enumerate(((gate_codes, gate_scale), (up_codes, up_scale))):
        unpack_tile(
            lambda g: codes[g * WORDS : (g + 1) * WORDS, :],
            lambda g: scale[where + (g // own, slice(g % own, g % own + 1), slice(None))],
            groups,
            dense[i],
        )
        out[:, i * part : (i + 1) * part] = dot(x[...], dense[i][...]).astype(jnp.bfloat16)


def project_shard(slot, x, codes, gate_scale, up_scale):
    tokens, depth = x.shape
    part = codes[0].shape[1]
    index = None if slot == 0 else slot - 1
    return local(
        functools.partial(shard_kernel, index=index),
        bf16(tokens, 2 * part),
        x, codes[2 * slot], codes[2 * slot + 1], gate_scale, up_scale,
        scratch=[pltpu.VMEM((depth, part), jnp.bfloat16)] * 2,
        flops=tokens * depth * part // 4,
        limit=20,
    )


def plus_kernel(a, b, out):
    out[...] = (a[...].astype(jnp.float32) + b[...].astype(jnp.float32)).astype(jnp.bfloat16)


def plus(a, b):
    return local(plus_kernel, bf16(*a.shape), a, b, flops=a.size)


def final_kernel(a, b, c, d, e, out):
    width = out.shape[1]
    order = group_order()
    for g in range(width // GROUP):
        gate_at = slice(g * GROUP, (g + 1) * GROUP)
        up_at = slice(width + g * GROUP, width + (g + 1) * GROUP)
        gate, up = (
            a[:, at].astype(jnp.float32)
            + b[:, at].astype(jnp.float32)
            + c[:, at].astype(jnp.float32)
            + d[:, at].astype(jnp.float32)
            + e[:, at].astype(jnp.float32)
            for at in (gate_at, up_at)
        )
        value = (gate / (1.0 + jnp.exp(-gate)) * up).astype(jnp.bfloat16)
        out[:, gate_at] = dot(value, order).astype(jnp.bfloat16)


def down_kernel_of(slot, parts, begin, last):
    def kernel(at, *refs):
        refs = list(refs)
        hidden, (codes, scale), refs = refs[:parts], refs[parts : parts + 2], refs[parts + 2 :]
        before = None if begin else refs.pop(0)
        dense, outs = refs[-1], refs[:-1]
        value = hidden[0][...]
        for ref in hidden[1:]:
            value = value + ref[...]
        depth = value.shape[1]
        words, groups = depth // CODES, depth // GROUP
        columns = codes.shape[1]
        half = value.shape[0] // 2
        first = at[COL] ^ MASKS[slot]
        for start in range(0, columns, columns // 4):
            lanes = slice(start, start + columns // 4)
            unpack_tile(
                lambda g: codes[pl.ds(pl.multiple_of(first * words + g * WORDS, WORDS), WORDS), lanes],
                lambda g: scale[first, g : g + 1, lanes],
                groups,
                dense.at[:, lanes],
            )
            total = dot(value, dense[:, lanes])
            if before is not None:
                total += before[:, lanes]
            if last:
                outs[0][:, lanes] = total[:half].astype(jnp.bfloat16)
                outs[1][:, lanes] = total[half:].astype(jnp.bfloat16)
            else:
                outs[0][:, lanes] = total

    return kernel


def down_shard(at, slot, hidden, codes, scale, before=None, last=False):
    tokens, depth = hidden[0].shape
    columns = codes.shape[1]
    if last:
        shapes = [bf16(tokens // 2, columns)] * 2
    else:
        shapes = jax.ShapeDtypeStruct((tokens, columns), jnp.float32)
    extra = () if before is None else (before,)
    return local(
        down_kernel_of(slot, len(hidden), before is None, last),
        shapes,
        at, *hidden, codes, scale, *extra,
        scalars=1,
        scratch=[pltpu.VMEM((depth, columns), jnp.bfloat16)],
        flops=tokens * depth * columns // 4,
    )


def pair_kernel(left, right, *outs):
    count = outs[0].shape[0]
    for b, out in enumerate(outs):
        rows = slice(b * count, (b + 1) * count)
        out[...] = (left[rows].astype(jnp.float32) + right[rows].astype(jnp.float32)).astype(jnp.bfloat16)


def total_kernel(*refs):
    total = refs[0][...].astype(jnp.float32)
    for ref in refs[1:-1]:
        total += ref[...].astype(jnp.float32)
    refs[-1][...] = total.astype(jnp.bfloat16)


def line_device(tokens, gate_codes, up_codes, down_codes, gate_scales, up_scales, down_scales):
    rows, cols = lax.axis_size("row"), lax.axis_size("col")
    row, col = lax.axis_index("row"), lax.axis_index("col")
    count, depth = tokens.shape
    own, hidden_units = gate_scales.shape[0], gate_codes.shape[1]
    part = hidden_units // cols
    features = down_codes.shape[1]
    down_groups = down_scales.shape[1] // rows
    at = jnp.stack([row // 2, row % 2, col]).astype(jnp.int32)

    def from_source(value, j):
        pairs = [(r * cols + r // 2, (r ^ (2 * j)) * cols + r // 2) for r in range(rows)]
        return lax.ppermute(value, ("row", "col"), pairs)

    first = local(
        functools.partial(first_kernel, part=part),
        [bf16(count + 2 * own, depth)] * 4,
        at, tokens, gate_scales, up_scales,
        scalars=1,
        remote=3,
        scratch=[
            pltpu.VMEM((count, depth), jnp.bfloat16),
            pltpu.SemaphoreType.DMA,
            pltpu.SemaphoreType.DMA((16,)),
        ],
    )
    mine = jnp.concatenate([first[0]] + [swap(first[j], "row", 2 * j) for j in range(1, 4)], axis=0)
    second = local(
        functools.partial(second_kernel, part=part),
        [bf16(2 * own, 6 * part)] * 4,
        at, gate_scales, up_scales,
        scalars=1,
        remote=2,
        scratch=[pltpu.SemaphoreType.DMA((48,))],
    )
    received = [from_source(second[j], j) for j in range(1, 4)]
    codes = local(
        stage_kernel,
        [jax.ShapeDtypeStruct((gate_codes.shape[0], part), jnp.int32)] * 8,
        at, gate_codes, up_codes,
        scalars=1,
        remote=2,
        scratch=[pltpu.SemaphoreType.DMA((8,))],
        flops=1 << 26,
    )
    other = swap(mine, "row", 1)
    scale = bf16(2, own, part)
    x, gate_scale, up_scale = local(
        functools.partial(gather_kernel, count=count, part=part),
        [bf16(rows * count, depth), scale, scale],
        at, mine, other,
        scalars=1,
    )

    s0 = project_shard(0, x, codes, gate_scale, up_scale)
    from_end = inward(s0)
    from_inner = across(s0)

    second = local(pick_kernel, bf16(*second[0].shape), at, second[0], *received, scalars=1)
    scale = bf16(3, 2, own, part)
    gate_rest, up_rest = local(
        functools.partial(spread_kernel, part=part),
        [scale, scale],
        at, second, swap(second, "row", 1),
        scalars=1,
    )
    s1 = project_shard(1, x, codes, gate_rest, up_rest)
    own_d = ends(s1)
    s2 = project_shard(2, x, codes, gate_rest, up_rest)
    own_a = inward(s2)
    s3 = project_shard(3, x, codes, gate_rest, up_rest)

    down_t = down_scales.T.reshape(rows // 2, 2 * down_groups, down_scales.shape[0])
    third = local(third_kernel, [bf16(*down_t.shape[1:])] * 4, at, down_t, scalars=1)
    received = [from_source(third[j], j) for j in range(1, 4)]
    third = local(pick_kernel, bf16(*third[0].shape), at, third[0], *received, scalars=1)
    down_scale = local(
        spread_down_kernel,
        bf16(cols, down_groups // cols, features),
        at, third, swap(third, "row", 1),
        scalars=1,
    )

    own_b = across(plus(s1, from_end))
    own_c = outward(plus(s2, from_inner))
    hidden = local(
        final_kernel,
        bf16(rows * count, part),
        s3, own_a, own_b, own_c, own_d,
        flops=rows * count * part * GROUP // 4,
    )

    to_inner = inward(hidden)
    between = across(hidden)
    to_end = outward(hidden)
    end_end = ends(hidden)
    far_inner = across(to_inner)
    far_end = outward(between)
    total = down_shard(at, 3, [hidden], down_codes, down_scale)
    total = down_shard(at, 2, [to_inner, to_end], down_codes, down_scale, total)
    total = down_shard(at, 1, [between, end_end], down_codes, down_scale, total)
    left, right = down_shard(at, 0, [far_inner, far_end], down_codes, down_scale, total, last=True)

    pair = local(pair_kernel, [bf16(count, features)] * 4, left, swap(right, "row", 1))
    return local(
        total_kernel,
        bf16(count, features),
        pair[0], *[swap(pair[b], "row", 2 * b) for b in range(1, 4)],
    )


def per_device(tokens, gate_codes, up_codes, down_codes, gate_scales, up_scales, down_scales):
    rows, cols = lax.axis_size("row"), lax.axis_size("col")
    sizes = (gate_codes.shape[1], down_scales.shape[0])
    fits = 2 * gate_codes.shape[1] <= tokens.shape[1] * cols and tokens.shape[0] % 16 == 0
    if cols == 4 and rows == 2 * cols and fits and all(n % (cols * 128) == 0 for n in sizes):
        return line_device(tokens, gate_codes, up_codes, down_codes, gate_scales, up_scales, down_scales)
    count = tokens.shape[0]
    mine = jnp.concatenate([tokens] + [swap(tokens, "row", d) for d in range(2, rows, 2)], axis=0)
    other = swap(mine, "row", 1)
    gate_scale, up_scale = input_scales((gate_scales, up_scales), gate_codes.shape[1])
    down_scale = output_scales(down_scales, down_codes.shape[1])
    partial = project(mine, other, gate_codes, up_codes, gate_scale, up_scale)
    down_dense = unpack_down(down_codes, down_scale)
    summed = lax.psum_scatter(partial, "col", scatter_dimension=0, tiled=True)
    hidden = lax.all_gather(activate(summed), "col", axis=0, tiled=True)
    result = down(hidden, down_dense)
    half = result.shape[0] // 2
    received = swap(result[half:], "row", 1)
    pair = (result[:half].astype(jnp.float32) + received.astype(jnp.float32)).astype(jnp.bfloat16)
    pieces = [pair[:count]] + [
        swap(pair[b * count : (b + 1) * count], "row", 2 * b) for b in range(1, rows // 2)
    ]
    total = pieces[0].astype(jnp.float32)
    for piece in pieces[1:]:
        total = total + piece.astype(jnp.float32)
    return total.astype(jnp.bfloat16)


def solution(mesh):
    placed = (
        P("row", "col"),
        P("col", "row"),
        P("col", "row"),
        P("row", "col"),
        P("row", None),
        P("row", None),
        P("row", None),
    )
    step = jax.shard_map(
        per_device, mesh=mesh, in_specs=placed, out_specs=P("row", "col"), check_vma=False
    )
    if mesh.shape["row"] == 2 * mesh.shape["col"]:
        return step
    return step
```

```python
import functools

import jax
import jax.numpy as jnp
from jax import lax
from jax.experimental import pallas as pl
from jax.experimental.pallas import tpu as pltpu
from jax.sharding import PartitionSpec as P


GROUP = 128
CODES = 8
WORDS = GROUP // CODES


def tile_of(length, most):
    tile = 128
    for width in range(128, most + 1, 128):
        if length % width == 0:
            tile = width
    return tile


def group_order():
    source = lax.broadcasted_iota(jnp.int32, (GROUP, GROUP), 0)
    target = lax.broadcasted_iota(jnp.int32, (GROUP, GROUP), 1)
    wanted = (target & (WORDS - 1)) * CODES + target // WORDS
    return jnp.where(source == wanted, 1.0, 0.0).astype(jnp.bfloat16)


def unpack_into(codes_ref, scale_ref, dense_ref):
    groups = codes_ref.shape[0] // WORDS
    for g in range(groups):
        words = codes_ref[g * WORDS : (g + 1) * WORDS, :]
        scale = scale_ref[g : g + 1, :]
        flipped = words ^ jnp.int32(-2004318072)
        for k in range(CODES):
            value = flipped if k == CODES - 1 else lax.shift_left(flipped, jnp.int32(28 - 4 * k))
            value = lax.shift_right_arithmetic(value, jnp.int32(28))
            rows = value.astype(jnp.float32).astype(jnp.bfloat16) * scale
            dense_ref[g * GROUP + k * WORDS : g * GROUP + (k + 1) * WORDS, :] = rows


def project_kernel(mine, other, gate_codes, up_codes, gate_scale, up_scale, out, x, gate_dense, up_dense):
    half = mine.shape[0]
    width = gate_codes.shape[1]

    @pl.when(pl.program_id(0) == 0)
    def _():
        order = group_order()
        for g in range(mine.shape[1] // GROUP):
            cols = slice(g * GROUP, (g + 1) * GROUP)
            x[:half, cols] = jnp.dot(mine[:, cols], order, preferred_element_type=jnp.float32).astype(jnp.bfloat16)
            x[half:, cols] = jnp.dot(other[:, cols], order, preferred_element_type=jnp.float32).astype(jnp.bfloat16)

    unpack_into(gate_codes, gate_scale, gate_dense)
    out[:, :width] = jnp.dot(x[...], gate_dense[...], preferred_element_type=jnp.float32).astype(jnp.bfloat16)
    unpack_into(up_codes, up_scale, up_dense)
    out[:, width:] = jnp.dot(x[...], up_dense[...], preferred_element_type=jnp.float32).astype(jnp.bfloat16)


def project(mine, other, gate_codes, up_codes, gate_scale, up_scale):
    words, hidden = gate_codes.shape
    depth = mine.shape[1]
    tokens = 2 * mine.shape[0]
    groups = gate_scale.shape[0]
    width = tile_of(hidden, 512)
    whole = lambda j: (0, 0)
    tile = lambda j: (0, j)
    return pl.pallas_call(
        project_kernel,
        grid=(hidden // width,),
        in_specs=[
            pl.BlockSpec(mine.shape, whole),
            pl.BlockSpec(other.shape, whole),
            pl.BlockSpec((words, width), tile),
            pl.BlockSpec((words, width), tile),
            pl.BlockSpec((groups, width), tile),
            pl.BlockSpec((groups, width), tile),
        ],
        out_specs=pl.BlockSpec((tokens, 2 * width), tile),
        out_shape=jax.ShapeDtypeStruct((tokens, 2 * hidden), jnp.bfloat16),
        scratch_shapes=[
            pltpu.VMEM((tokens, depth), jnp.bfloat16),
            pltpu.VMEM((depth, width), jnp.bfloat16),
            pltpu.VMEM((depth, width), jnp.bfloat16),
        ],
        cost_estimate=pl.CostEstimate(
            flops=4 * tokens * depth * hidden, bytes_accessed=8 * words * hidden, transcendentals=0
        ),
    )(mine, other, gate_codes, up_codes, gate_scale, up_scale)


def hidden_kernel(sums, out):
    width = out.shape[1]
    gate = sums[:, :width].astype(jnp.float32)
    up = sums[:, width:].astype(jnp.float32)
    value = (gate / (1.0 + jnp.exp(-gate)) * up).astype(jnp.bfloat16)
    order = group_order()
    for g in range(width // GROUP):
        cols = slice(g * GROUP, (g + 1) * GROUP)
        out[:, cols] = jnp.dot(value[:, cols], order, preferred_element_type=jnp.float32).astype(jnp.bfloat16)


def activate(sums):
    tokens, columns = sums.shape
    hidden = columns // 2
    width = tile_of(hidden, 512)
    return pl.pallas_call(
        hidden_kernel,
        grid=(hidden // width,),
        in_specs=[pl.BlockSpec((tokens, 2 * width), lambda j: (0, j))],
        out_specs=pl.BlockSpec((tokens, width), lambda j: (0, j)),
        out_shape=jax.ShapeDtypeStruct((tokens, hidden), jnp.bfloat16),
        cost_estimate=pl.CostEstimate(
            flops=2 * tokens * hidden * GROUP, bytes_accessed=6 * tokens * hidden, transcendentals=tokens * hidden
        ),
    )(sums)


def unpack_kernel(codes, scale, out):
    unpack_into(codes, scale, out)


def unpack_down(codes, scale):
    words, columns = codes.shape
    width = tile_of(columns, 256)
    tile = lambda j: (0, j)
    return pl.pallas_call(
        unpack_kernel,
        grid=(columns // width,),
        in_specs=[pl.BlockSpec((words, width), tile), pl.BlockSpec((scale.shape[0], width), tile)],
        out_specs=pl.BlockSpec((words * CODES, width), tile),
        out_shape=jax.ShapeDtypeStruct((words * CODES, columns), jnp.bfloat16),
        cost_estimate=pl.CostEstimate(
            flops=8 * words * CODES * columns, bytes_accessed=20 * words * columns, transcendentals=0
        ),
    )(codes, scale)


def down_kernel(hidden, dense, out):
    out[...] = jnp.dot(hidden[...], dense[...], preferred_element_type=jnp.float32).astype(jnp.bfloat16)


def down(hidden, dense):
    tokens, depth = hidden.shape
    columns = dense.shape[1]
    width = tile_of(columns, 512)
    return pl.pallas_call(
        down_kernel,
        grid=(columns // width,),
        in_specs=[pl.BlockSpec(hidden.shape, lambda j: (0, 0)), pl.BlockSpec((depth, width), lambda j: (0, j))],
        out_specs=pl.BlockSpec((tokens, width), lambda j: (0, j)),
        out_shape=jax.ShapeDtypeStruct((tokens, columns), jnp.bfloat16),
        cost_estimate=pl.CostEstimate(
            flops=2 * tokens * depth * columns, bytes_accessed=2 * depth * columns, transcendentals=0
        ),
    )(hidden, dense)


def swap(value, axis, distance):
    count = lax.axis_size(axis)
    return lax.ppermute(value, axis, [(i, i ^ distance) for i in range(count)])


def input_scales(scales, hidden):
    rows, cols, col = lax.axis_size("row"), lax.axis_size("col"), lax.axis_index("col")
    part = hidden // cols
    sent = jnp.stack(
        [
            jnp.stack([lax.dynamic_slice_in_dim(s, r * hidden + col * part, part, 1) for s in scales])
            for r in range(rows)
        ]
    )
    got = lax.all_to_all(sent, "row", split_axis=0, concat_axis=0, tiled=True)
    own = got.shape[2]
    got = got.reshape(cols, rows // cols, len(scales), own, part)
    got = lax.all_to_all(got, "col", split_axis=0, concat_axis=0, tiled=True)
    got = got.transpose(2, 1, 3, 0, 4).reshape(len(scales), rows // cols * own, hidden)
    return [got[i] for i in range(len(scales))]


def output_scales(scales, model_cols):
    rows, cols, col = lax.axis_size("row"), lax.axis_size("col"), lax.axis_index("col")
    features, groups = scales.shape
    part = features // cols
    mine = lax.dynamic_slice_in_dim(scales, col * part, part, 0).T
    got = lax.all_to_all(
        mine.reshape(rows, groups // rows, part), "row", split_axis=0, concat_axis=0, tiled=True
    )
    got = got.reshape(cols, rows // cols, groups // rows, part)
    got = lax.all_to_all(got, "col", split_axis=0, concat_axis=0, tiled=True)
    return got.transpose(2, 1, 0, 3).reshape(groups // rows, model_cols)


VMEM = pl.BlockSpec(memory_space=pltpu.VMEM)
SMEM = pl.BlockSpec(memory_space=pltpu.SMEM)
HBM = pl.BlockSpec(memory_space=pltpu.HBM)


def local(kernel, shapes, *args, scalars=0, remote=0, scratch=(), flops=0, limit=16):
    several = isinstance(shapes, list)
    args = list(args)
    for i in range(scalars, scalars + remote):
        args[i] = pltpu.with_memory_space_constraint(args[i], pltpu.HBM)
    return pl.pallas_call(
        kernel,
        in_specs=[SMEM] * scalars + [HBM] * remote + [VMEM] * (len(args) - scalars - remote),
        out_specs=[VMEM] * len(shapes) if several else VMEM,
        out_shape=shapes,
        scratch_shapes=list(scratch),
        compiler_params=pltpu.CompilerParams(vmem_limit_bytes=limit << 20),
        cost_estimate=pl.CostEstimate(flops=flops, bytes_accessed=0, transcendentals=0),
    )(*args)


def bf16(*shape):
    return jax.ShapeDtypeStruct(shape, jnp.bfloat16)


def inward(value):
    return lax.ppermute(value, "col", [(0, 1), (3, 2)])


def across(value):
    return lax.ppermute(value, "col", [(1, 2), (2, 1)])


def outward(value):
    return lax.ppermute(value, "col", [(2, 3), (1, 0)])


def ends(value):
    return lax.ppermute(value, "col", [(0, 3), (3, 0)])


def lanes_at(start, size):
    return pl.ds(pl.multiple_of(start, 128), size)


def dot(a, b):
    return jnp.dot(a, b, preferred_element_type=jnp.float32)


CHIP, CORE, COL = 0, 1, 2

MASKS = (2, 3, 1, 0)


def first_kernel(at, tokens, gate, up, *refs, part):
    outs, (held, arrived, sems) = refs[:4], refs[4:]
    count, own = tokens.shape[0], gate.shape[0]
    fetch = pltpu.make_async_copy(tokens, held, arrived)
    fetch.start()
    copies = []
    for j, out in enumerate(outs):
        for core in range(2):
            start = (((at[CHIP] ^ j) * 2 + core) * 4 + (at[COL] ^ MASKS[0])) * part
            for i, scale in enumerate((gate, up)):
                rows = slice(count + i * own, count + (i + 1) * own)
                copies.append(
                    pltpu.make_async_copy(
                        scale.at[:, lanes_at(start, part)],
                        out.at[rows, core * part : (core + 1) * part],
                        sems.at[len(copies)],
                    )
                )
                copies[-1].start()
    order = group_order()
    fetch.wait()
    for g in range(tokens.shape[1] // GROUP):
        lanes = slice(g * GROUP, (g + 1) * GROUP)
        value = dot(held[:, lanes], order).astype(jnp.bfloat16)
        for out in outs:
            out[:count, lanes] = value
    for copy in copies:
        copy.wait()


def second_kernel(at, gate, up, *refs, part):
    outs, sems = refs[:-1], refs[-1]
    own = gate.shape[0]
    copies = []
    for j, out in enumerate(outs):
        for core in range(2):
            for slot in range(1, 4):
                start = (((at[CHIP] ^ j) * 2 + core) * 4 + (at[COL] ^ MASKS[slot])) * part
                lanes = slice(((slot - 1) * 2 + core) * part, ((slot - 1) * 2 + core + 1) * part)
                for i, scale in enumerate((gate, up)):
                    copies.append(
                        pltpu.make_async_copy(
                            scale.at[:, lanes_at(start, part)],
                            out.at[i * own : (i + 1) * own, lanes],
                            sems.at[len(copies)],
                        )
                    )
                    copies[-1].start()
    for copy in copies:
        copy.wait()


def third_kernel(at, down_t, *outs):
    for j, out in enumerate(outs):
        out[...] = down_t[at[CHIP] ^ j]


def stage_kernel(at, gate, up, *refs, masks):
    outs, sems = refs[:-1], refs[-1]
    part = gate.shape[1] // 4
    copies = []
    for slot, mask in enumerate(masks):
        lanes = lanes_at((at[COL] ^ mask) * part, part)
        for i, codes in enumerate((gate, up)):
            index = 2 * slot + i
            copies.append(pltpu.make_async_copy(codes.at[:, lanes], outs[index], sems.at[index]))
            copies[-1].start()
    for copy in copies:
        copy.wait()


def gather_kernel(at, mine, other, x, gate, up, *, count, part):
    block = mine.shape[0] // 4
    half = x.shape[0] // 2
    own = gate.shape[1]
    for i, j in enumerate((2, 3, 0, 1)):
        start = i // 2 * half + i % 2 * count
        x[start : start + count, :] = mine[j * block : j * block + count, :]
        x[start + half // 2 : start + half // 2 + count, :] = other[j * block : j * block + count, :]
    source = (at[CHIP] ^ at[COL]) * block + count
    rows = pl.ds(pl.multiple_of(source, 16), 2 * own)
    lanes = lanes_at(at[CORE] * part, part)
    for core, ref in ((at[CORE], mine), (1 - at[CORE], other)):
        both = ref[rows, lanes]
        gate[core] = both[:own]
        up[core] = both[own:]


def pick_kernel(at, own, *refs):
    received, out = refs[:-1], refs[-1]
    keep = at[CHIP] == at[COL]

    @pl.when(keep)
    def _():
        out[...] = own[...]

    @pl.when(jnp.logical_not(keep))
    def _():
        total = received[0][...]
        for ref in received[1:]:
            total += ref[...]
        out[...] = total


def spread_kernel(at, mine, other, gate, up, *, part):
    own = gate.shape[2]
    for core, ref in ((at[CORE], mine), (1 - at[CORE], other)):
        for slot in range(3):
            lanes = lanes_at((slot * 2 + at[CORE]) * part, part)
            gate[slot, core] = ref[:own, lanes]
            up[slot, core] = ref[own:, lanes]


def spread_down_kernel(at, mine, other, out):
    shards, groups, features = out.shape
    width = features // 2
    for core, ref in ((at[CORE], mine), (1 - at[CORE], other)):
        rows = ref[...].astype(jnp.float32)
        value = jnp.where(at[CORE] == 0, rows[: shards * groups], rows[shards * groups :]).astype(jnp.bfloat16)
        for shard in range(shards):
            out[shard, :, lanes_at(core * width, width)] = value[shard * groups : (shard + 1) * groups]


def unpack_tile(codes, scale, groups, dense):
    for g in range(groups):
        words = codes(g) ^ jnp.int32(-2004318072)
        factor = jnp.broadcast_to(scale(g), (WORDS, words.shape[1]))
        for k in range(CODES):
            value = words if k == CODES - 1 else lax.shift_left(words, jnp.int32(28 - 4 * k))
            value = lax.shift_right_arithmetic(value, jnp.int32(28))
            rows = slice(g * GROUP + k * WORDS, g * GROUP + (k + 1) * WORDS)
            dense[rows, :] = value.astype(jnp.float32).astype(jnp.bfloat16) * factor


def shard_kernel(x, gate_codes, up_codes, gate_scale, up_scale, early, late, *dense, index):
    part = gate_codes.shape[1]
    own = gate_scale.shape[-2]
    groups = gate_codes.shape[0] // WORDS
    where = () if index is None else (index,)
    for i, (codes, scale) in enumerate(((gate_codes, gate_scale), (up_codes, up_scale))):
        unpack_tile(
            lambda g: codes[g * WORDS : (g + 1) * WORDS, :],
            lambda g: scale[where + (g // own, slice(g % own, g % own + 1), slice(None))],
            groups,
            dense[i],
        )
        value = dot(x[...], dense[i][...]).astype(jnp.bfloat16)
        half = value.shape[0] // 2
        early[:, i * part : (i + 1) * part] = value[:half]
        late[:, i * part : (i + 1) * part] = value[half:]


def project_shard(slot, x, codes, gate_scale, up_scale):
    tokens, depth = x.shape
    part = codes[0].shape[1]
    index = None if slot == 0 else slot - 1
    return local(
        functools.partial(shard_kernel, index=index),
        [bf16(tokens // 2, 2 * part)] * 2,
        x, codes[2 * slot], codes[2 * slot + 1], gate_scale, up_scale,
        scratch=[pltpu.VMEM((depth, part), jnp.bfloat16)] * 2,
        flops=tokens * depth * part // 4,
        limit=20,
    )


def plus_kernel(a, b, out):
    out[...] = (a[...].astype(jnp.float32) + b[...].astype(jnp.float32)).astype(jnp.bfloat16)


def plus(a, b):
    return local(plus_kernel, bf16(*a.shape), a, b, flops=a.size)


def final_kernel(*refs):
    sums, out = refs[:-1], refs[-1]
    width = out.shape[1]
    order = group_order()
    for g in range(width // GROUP):
        gate_at = slice(g * GROUP, (g + 1) * GROUP)
        up_at = slice(width + g * GROUP, width + (g + 1) * GROUP)
        gate, up = (sum(ref[:, at].astype(jnp.float32) for ref in sums) for at in (gate_at, up_at))
        value = (gate / (1.0 + jnp.exp(-gate)) * up).astype(jnp.bfloat16)
        out[:, gate_at] = dot(value, order).astype(jnp.bfloat16)


def add_all(refs):
    value = refs[0][...]
    for ref in refs[1:]:
        value = value + ref[...]
    return value


def put(outs, lanes, total):
    if len(outs) == 1:
        outs[0][:, lanes] = total
    else:
        half = total.shape[0] // 2
        outs[0][:, lanes] = total[:half].astype(jnp.bfloat16)
        outs[1][:, lanes] = total[half:].astype(jnp.bfloat16)


def unpack_down_kernel(at, codes, scale, dense, *, slot):
    words, groups = dense.shape[0] // CODES, dense.shape[0] // GROUP
    columns = codes.shape[1]
    first = at[COL] ^ MASKS[slot]
    for start in range(0, columns, columns // 4):
        lanes = slice(start, start + columns // 4)
        unpack_tile(
            lambda g: codes[pl.ds(pl.multiple_of(first * words + g * WORDS, WORDS), WORDS), lanes],
            lambda g: scale[first, g : g + 1, lanes],
            groups,
            dense.at[:, lanes],
        )


def dense_down_kernel(*refs, parts, begin):
    refs = list(refs)
    hidden, dense, refs = refs[:parts], refs[parts], refs[parts + 1 :]
    before = None if begin else refs.pop(0)
    value = add_all(hidden)
    columns = dense.shape[1]
    for start in range(0, columns, columns // 4):
        lanes = slice(start, start + columns // 4)
        total = dot(value, dense[:, lanes])
        if before is not None:
            total += before[:, lanes]
        put(refs, lanes, total)


def down_shapes(tokens, columns, last):
    if last:
        return [bf16(tokens // 2, columns)] * 2
    return [jax.ShapeDtypeStruct((tokens, columns), jnp.float32)]


def unpack_down_shard(at, slot, codes, scale):
    depth, columns = codes.shape[0] * CODES // 4, codes.shape[1]
    return local(
        functools.partial(unpack_down_kernel, slot=slot),
        bf16(depth, columns),
        at, codes, scale,
        scalars=1,
        flops=depth * columns * 16,
    )


def dense_down_shard(hidden, dense, before, last):
    tokens, depth = hidden[0].shape
    return local(
        functools.partial(dense_down_kernel, parts=len(hidden), begin=before is None),
        down_shapes(tokens, dense.shape[1], last),
        *hidden, dense, *(() if before is None else (before,)),
        flops=tokens * depth * dense.shape[1] // 8,
    )


def pair_kernel(left, right, *outs):
    count = outs[0].shape[0]
    for b, out in enumerate(outs):
        rows = slice(b * count, (b + 1) * count)
        out[...] = (left[rows].astype(jnp.float32) + right[rows].astype(jnp.float32)).astype(jnp.bfloat16)


def total_kernel(*refs):
    total = refs[0][...].astype(jnp.float32)
    for ref in refs[1:-1]:
        total += ref[...].astype(jnp.float32)
    refs[-1][...] = total.astype(jnp.bfloat16)


def line_device(tokens, gate_codes, up_codes, down_codes, gate_scales, up_scales, down_scales):
    rows, cols = lax.axis_size("row"), lax.axis_size("col")
    row, col = lax.axis_index("row"), lax.axis_index("col")
    count, depth = tokens.shape
    own, hidden_units = gate_scales.shape[0], gate_codes.shape[1]
    part = hidden_units // cols
    features = down_codes.shape[1]
    down_groups = down_scales.shape[1] // rows
    at = jnp.stack([row // 2, row % 2, col]).astype(jnp.int32)

    def from_source(value, j):
        pairs = [(r * cols + r // 2, (r ^ (2 * j)) * cols + r // 2) for r in range(rows)]
        return lax.ppermute(value, ("row", "col"), pairs)

    first = local(
        functools.partial(first_kernel, part=part),
        [bf16(count + 2 * own, depth)] * 4,
        at, tokens, gate_scales, up_scales,
        scalars=1,
        remote=3,
        scratch=[
            pltpu.VMEM((count, depth), jnp.bfloat16),
            pltpu.SemaphoreType.DMA,
            pltpu.SemaphoreType.DMA((16,)),
        ],
    )
    mine = jnp.concatenate([first[0]] + [swap(first[j], "row", 2 * j) for j in range(1, 4)], axis=0)
    second = local(
        functools.partial(second_kernel, part=part),
        [bf16(2 * own, 6 * part)] * 4,
        at, gate_scales, up_scales,
        scalars=1,
        remote=2,
        scratch=[pltpu.SemaphoreType.DMA((48,))],
    )
    received = [from_source(second[j], j) for j in range(1, 4)]

    def stage(masks, flops):
        return local(
            functools.partial(stage_kernel, masks=masks),
            [jax.ShapeDtypeStruct((gate_codes.shape[0], part), jnp.int32)] * (2 * len(masks)),
            at, gate_codes, up_codes,
            scalars=1,
            remote=2,
            scratch=[pltpu.SemaphoreType.DMA((2 * len(masks),))],
            flops=flops,
        )

    codes = [*stage(MASKS[:2], 1 << 25), *stage(MASKS[2:], 1 << 25)]
    other = swap(mine, "row", 1)
    scale = bf16(2, own, part)
    x, gate_scale, up_scale = local(
        functools.partial(gather_kernel, count=count, part=part),
        [bf16(rows * count, depth), scale, scale],
        at, mine, other,
        scalars=1,
    )

    a0, b0 = project_shard(0, x, codes, gate_scale, up_scale)
    a_inner = inward(a0)
    a_near = across(a0)

    second = local(pick_kernel, bf16(*second[0].shape), at, second[0], *received, scalars=1)
    scale = bf16(3, 2, own, part)
    gate_rest, up_rest = local(
        functools.partial(spread_kernel, part=part),
        [scale, scale],
        at, second, swap(second, "row", 1),
        scalars=1,
    )
    a1, b1 = project_shard(1, x, codes, gate_rest, up_rest)
    a_end = ends(a1)
    a2, b2 = project_shard(2, x, codes, gate_rest, up_rest)
    a_own = inward(a2)
    a3, b3 = project_shard(3, x, codes, gate_rest, up_rest)
    a_across = across(plus(a1, a_inner))
    a_out = outward(plus(a2, a_near))

    down_t = down_scales.T.reshape(rows // 2, 2 * down_groups, down_scales.shape[0])
    third = local(third_kernel, [bf16(*down_t.shape[1:])] * 4, at, down_t, scalars=1)
    received = [from_source(third[j], j) for j in range(1, 4)]
    third = local(pick_kernel, bf16(*third[0].shape), at, third[0], *received, scalars=1)
    down_scale = local(
        spread_down_kernel,
        bf16(cols, down_groups // cols, features),
        at, third, swap(third, "row", 1),
        scalars=1,
    )

    half = rows * count // 2

    def activate_sums(*sums):
        return local(final_kernel, bf16(half, part), *sums, flops=half * part * GROUP // 4)

    b_far = inward(b1)
    b_inner = inward(b0)
    b_own = inward(b2)
    b_chain = across(plus(b0, b_far))
    b_across = across(plus(b1, b_inner))
    b_out = outward(plus(b2, b_chain))

    ha = activate_sums(a3, a_own, a_across, a_out, a_end)
    a_to_inner = inward(ha)
    a_between = across(ha)
    a_to_end = outward(ha)
    a_far_inner = across(a_to_inner)
    a_far_end = outward(a_between)
    a_end_end = outward(a_far_inner)

    hb = activate_sums(b3, b_own, b_across, b_out)
    b_to_inner = inward(hb)
    b_between = across(hb)
    b_to_end = outward(hb)
    b_end_end = ends(hb)
    b_far_inner = across(b_to_inner)
    b_far_end = outward(b_between)

    weights = [unpack_down_shard(at, slot, down_codes, down_scale) for slot in range(len(MASKS))]

    def down_all(*steps):
        total = None
        for i, (slot, parts) in enumerate(steps):
            last = i == len(steps) - 1
            rest = dense_down_shard(parts, weights[slot], total, last)
            total = rest[0]
        return rest

    def join(left, right):
        return local(pair_kernel, [bf16(count, features)] * 2, left, swap(right, "row", 1))

    near_a, far_a = (2, [a_to_inner, a_to_end]), (0, [a_far_inner, a_far_end])
    pair_a = join(*down_all((3, [ha]), near_a, far_a, (1, [a_between, a_end_end])))
    from_a = [swap(piece, "row", 2 * j) for j, piece in zip((2, 3), pair_a)]
    near_b, far_b = (2, [b_to_inner, b_to_end]), (0, [b_far_inner, b_far_end])
    pair_b = join(*down_all((3, [hb]), near_b, (1, [b_between, b_end_end]), far_b))
    return local(total_kernel, bf16(count, features), pair_b[0], *from_a, swap(pair_b[1], "row", 2))


def per_device(tokens, gate_codes, up_codes, down_codes, gate_scales, up_scales, down_scales):
    rows, cols = lax.axis_size("row"), lax.axis_size("col")
    sizes = (gate_codes.shape[1], down_scales.shape[0])
    fits = 2 * gate_codes.shape[1] <= tokens.shape[1] * cols and tokens.shape[0] % 16 == 0
    if cols == 4 and rows == 2 * cols and fits and all(n % (cols * 128) == 0 for n in sizes):
        return line_device(tokens, gate_codes, up_codes, down_codes, gate_scales, up_scales, down_scales)
    count = tokens.shape[0]
    mine = jnp.concatenate([tokens] + [swap(tokens, "row", d) for d in range(2, rows, 2)], axis=0)
    other = swap(mine, "row", 1)
    gate_scale, up_scale = input_scales((gate_scales, up_scales), gate_codes.shape[1])
    down_scale = output_scales(down_scales, down_codes.shape[1])
    partial = project(mine, other, gate_codes, up_codes, gate_scale, up_scale)
    down_dense = unpack_down(down_codes, down_scale)
    summed = lax.psum_scatter(partial, "col", scatter_dimension=0, tiled=True)
    hidden = lax.all_gather(activate(summed), "col", axis=0, tiled=True)
    result = down(hidden, down_dense)
    half = result.shape[0] // 2
    received = swap(result[half:], "row", 1)
    pair = (result[:half].astype(jnp.float32) + received.astype(jnp.float32)).astype(jnp.bfloat16)
    pieces = [pair[:count]] + [
        swap(pair[b * count : (b + 1) * count], "row", 2 * b) for b in range(1, rows // 2)
    ]
    total = pieces[0].astype(jnp.float32)
    for piece in pieces[1:]:
        total = total + piece.astype(jnp.float32)
    return total.astype(jnp.bfloat16)


def solution(mesh):
    placed = (
        P("row", "col"),
        P("col", "row"),
        P("col", "row"),
        P("row", "col"),
        P("row", None),
        P("row", None),
        P("row", None),
    )
    step = jax.shard_map(
        per_device, mesh=mesh, in_specs=placed, out_specs=P("row", "col"), check_vma=False
    )
    if mesh.shape["row"] == 2 * mesh.shape["col"]:
        return step
    return step
```
